32 devices in a mesh: groups: 2 (over x), blk: 8 (over z, y), rep: 2 (over core).
Axes of the slice: x: 2, y: 2, z: 4, core: 2. Of those that a mesh axis runs over, the one named last changes fastest.
Arguments:
- resident: bfloat16 [32768, 768], P(('groups', 'blk', 'rep')), parts along dimension 0, may hold values from -600 to 600
- ingest: bfloat16 [16384, 768], P(('groups', 'blk', 'rep')), parts along dimension 0, may hold values from -600 to 600
- cluster_ids: int32 [16384], P(('groups', 'blk', 'rep')), parts along dimension 0, may hold values from 0 to 127, as said below
Outputs:
- resident_score: float32 [32768], P(('groups', 'blk', 'rep')), parts along dimension 0
- ingest_score: float32 [16384], P(('groups', 'blk', 'rep')), parts along dimension 0
The draws below stay inside these ranges and needn't reach their ends.
There are 2 independent parts, one for each index of `groups`. The reference program is written for one: setup_inputs(seed, part) draws one part's arguments, and reference() takes and returns one part's arrays. A program takes and returns all parts, laid end to end along the dimension named above; each array names one. Nothing has to cross between parts.
Inputs may be any that keep to these rules, and one draw needn't show every extreme that they name: `cluster_ids`: clusters 16 * p to 16 * p + 15 belong to cycle position p. At most 96 documents of one device belong to one cycle position, and in every draw some cycle position receives 96 from every device.
All inputs are finite; a program needn't handle non-finite values.
Results may differ from the reference program's by a relative error of at most 0.0003.
Values may be sent and summed in bfloat16 or wider, within the bound.
A program may use at most 64 MiB of HBM per device.

```python
import jax
import jax.numpy as jnp
from jax import lax

D = 768
INGEST_DEV = 512
CL_OWN = 16
CYCLE_STEPS = 4
CAP = 96
VISIT = 1536
RES_POS = 2048
RESIDENT = 16384
INGEST = 8192
CLUSTERS = 128
N_BLK = 8
N_REP = 2


def slot_layout(key):
    base = jax.random.fold_in(key, 7)
    sources = N_BLK * N_REP
    slot_total = N_BLK * CAP
    weights = jax.random.randint(jax.random.fold_in(base, 1), (N_BLK,), 1, 9)
    heavy = jax.random.randint(jax.random.fold_in(base, 2), (), 0, N_BLK)
    raw = jax.random.randint(jax.random.fold_in(base, 3), (sources, N_BLK, CAP), 0, 1024) * weights[None, :, None]
    owner_grid = jnp.arange(N_BLK, dtype=jnp.int32)[None, :, None]
    raw = raw + jnp.where(owner_grid == heavy, 16384, 0)
    ordering = jnp.arange(slot_total, dtype=jnp.int32).reshape(1, N_BLK, CAP)
    scores = (raw * slot_total + ordering).reshape(sources, slot_total)
    chosen = lax.top_k(scores, INGEST_DEV)[1]
    shuffle_bits = jax.random.randint(jax.random.fold_in(base, 4), (sources, INGEST_DEV), 0, 2 ** 20)
    shuffle_keys = shuffle_bits * INGEST_DEV + jnp.arange(INGEST_DEV, dtype=jnp.int32)[None, :]
    shuffled = jnp.take_along_axis(chosen, jnp.argsort(shuffle_keys, axis=1), axis=1)
    owners = shuffled // CAP
    within = jax.random.randint(jax.random.fold_in(base, 5), (sources, INGEST_DEV), 0, CL_OWN)
    return (owners * CL_OWN + within).reshape(-1).astype(jnp.int32)


def centroid_table(key):
    base = jax.random.fold_in(key, 101)
    span = 6 * CL_OWN
    basis = jax.random.truncated_normal(jax.random.fold_in(base, 1), -5.0, 5.0, (CLUSTERS, D), jnp.float32)
    indices = jnp.arange(CLUSTERS, dtype=jnp.int32)
    band = ((indices[None, :] - indices[:, None]) % CLUSTERS < span).astype(jnp.float32)
    centres = jnp.dot(band, basis, precision=lax.Precision.HIGHEST) / jnp.sqrt(jnp.float32(min(span, CLUSTERS)))
    spread = jnp.exp(jax.random.uniform(jax.random.fold_in(base, 2), (CLUSTERS,), jnp.float32, jnp.log(0.4), jnp.log(2.0)))
    return (centres, spread)


def embed_rows(key, clusters, salt):
    centres, spread = centroid_table(key)
    salted = jax.random.fold_in(key, salt)
    count = clusters.shape[0]
    jitter = jax.random.truncated_normal(jax.random.fold_in(salted, 1), -5.0, 5.0, (count, D), jnp.float32)
    scales = jnp.exp(jax.random.uniform(jax.random.fold_in(salted, 2), (count,), jnp.float32, 0.0, jnp.log(10.0)))
    rows = (0.5 * centres[clusters] + spread[clusters][:, None] * jitter) * scales[:, None]
    return rows.astype(jnp.bfloat16)


def draw_resident(key, part):
    positions = jnp.arange(RESIDENT, dtype=jnp.int32) // RES_POS
    within = jax.random.randint(jax.random.fold_in(key, 201), (RESIDENT,), 0, CL_OWN)
    return embed_rows(key, positions * CL_OWN + within, 202)


def draw_ingest(key, part):
    clusters = slot_layout(key)
    rows = embed_rows(key, clusters, 203).astype(jnp.float32)
    resident_rows = draw_resident(key, part).astype(jnp.float32)
    base = jax.random.fold_in(key, 301)
    owners = clusters // CL_OWN
    offsets = jax.random.randint(jax.random.fold_in(base, 1), (INGEST,), 1, CYCLE_STEPS + 1)
    picks = jax.random.randint(jax.random.fold_in(base, 2), (INGEST,), 0, RES_POS)
    sources = (owners + offsets) % N_BLK * RES_POS + picks
    copied = resident_rows[sources]
    level = jnp.sqrt(jnp.mean(copied * copied, axis=1) + 1e-12)
    noise = jax.random.truncated_normal(jax.random.fold_in(base, 3), -3.0, 3.0, (INGEST, D), jnp.float32)
    factor = jax.random.uniform(jax.random.fold_in(base, 4), (INGEST,), jnp.float32, 0.5, 1.0)
    near = (copied + 0.02 * level[:, None] * noise) * factor[:, None]
    planted = jax.random.randint(jax.random.fold_in(base, 5), (INGEST,), 0, 4) == 0
    rows = jnp.where(planted[:, None], near, rows)
    return rows.astype(jnp.bfloat16)


def draw_cluster_ids(key, part):
    return slot_layout(key)


def setup_inputs(seed: int = 0, part: int = 0) -> dict:
    splits = jax.random.split(jax.random.key(seed), 4)
    part_keys = jax.random.split(jax.random.fold_in(splits[3], part), 4)
    resident = draw_resident(jax.random.fold_in(jax.random.fold_in(splits[3], part), 71), part)
    ingest = draw_ingest(jax.random.fold_in(jax.random.fold_in(splits[3], part), 71), part)
    cluster_ids = draw_cluster_ids(jax.random.fold_in(jax.random.fold_in(splits[3], part), 71), part)
    return {"resident": resident, "ingest": ingest, "cluster_ids": cluster_ids}


temper = 0.2
epsilon = 1e-06

def unit_rows(rows):
    values = rows.astype(jnp.float32)
    squares = lax.optimization_barrier(jnp.sum(values * values, axis=-1, keepdims=True)) + epsilon
    factor = lax.rsqrt(squares)
    return (values * factor).astype(jnp.bfloat16)

def reference(resident, ingest, cluster_ids):
    unit_resident = unit_rows(resident).reshape(N_BLK, RES_POS, D)
    unit_ingest = unit_rows(ingest)
    owners = cluster_ids // CL_OWN
    sources = N_BLK * N_REP
    grouped = owners.reshape(sources, INGEST_DEV)
    onehot = (grouped[:, :, None] == jnp.arange(N_BLK, dtype=jnp.int32)[None, None, :]).astype(jnp.int32)
    rank_within = lax.optimization_barrier(jnp.sum((jnp.cumsum(onehot, axis=1) - onehot) * onehot, axis=2))
    source_ids = jnp.arange(sources, dtype=jnp.int32)[:, None]
    slot_index = (source_ids % N_REP * (N_BLK * CAP) + source_ids // N_REP * CAP + rank_within).reshape(INGEST)
    visiting = jnp.zeros((N_BLK, VISIT, D), jnp.bfloat16).at[owners, slot_index].set(unit_ingest)
    occupied = jnp.zeros((N_BLK, VISIT), jnp.float32).at[owners, slot_index].set(1.0)

    def per_owner(pieces):
        position, visitors, occupancy = pieces
        visit_sum = jnp.zeros((VISIT,), jnp.float32)
        partials = []
        for offset in range(CYCLE_STEPS + 1):
            resident_block = lax.dynamic_index_in_dim(unit_resident, (position + offset) % N_BLK, 0, keepdims=False)
            scores = jnp.dot(visitors, resident_block.T, preferred_element_type=jnp.float32)
            kernel = jnp.exp((scores - 1.0) / temper)
            visit_sum = visit_sum + lax.optimization_barrier(jnp.sum(kernel, axis=1))
            partials.append(lax.optimization_barrier(jnp.sum(kernel * occupancy[:, None], axis=0)))
        return (visit_sum, jnp.stack(partials))
    visit_sums, resident_parts = lax.map(per_owner, (jnp.arange(N_BLK, dtype=jnp.int32), visiting, occupied))
    resident_density = resident_parts[:, 0]
    for offset in range(1, CYCLE_STEPS + 1):
        resident_density = resident_density + jnp.roll(resident_parts[:, offset], offset, axis=0)
    ingest_density = visit_sums[owners, slot_index]
    return (jnp.log1p(resident_density.reshape(RESIDENT)), jnp.log1p(ingest_density))
```

```python
import functools
import math

import jax
import jax.numpy as jnp
from jax import lax
from jax.experimental import pallas as pl
from jax.experimental.pallas import tpu as pltpu
from jax.sharding import PartitionSpec as P

INGEST_DEV = 512
CL_OWN = 16
CYCLE_STEPS = 4


temper = 0.2
epsilon = 1e-06


def shifted(value, axis, steps):
    count = lax.axis_size(axis)
    pairs = [(source, (source + steps) % count) for source in range(count)]
    return lax.ppermute(value, axis, pairs)


def unit_rows(rows):
    values = rows.astype(jnp.float32)
    squares = jnp.sum(values * values, axis=-1, keepdims=True) + epsilon
    factor = lax.rsqrt(squares)
    return (values * factor).astype(jnp.bfloat16)


def kernel_sums(visitors, occupancy, residents):
    count_rows = visitors.shape[0]
    block_rows = 512
    num_blocks = count_rows // block_rows
    visit_blocks = visitors.reshape(num_blocks, block_rows, visitors.shape[1])
    live_blocks = occupancy.astype(jnp.float32).reshape(num_blocks, block_rows)

    def tile_sums(running, pieces):
        visit_tile, live_tile = pieces
        scores = jnp.einsum("vd,rd->vr", visit_tile, residents, preferred_element_type=jnp.float32)
        kernel = jnp.exp((scores - 1.0) / temper)
        return (running + jnp.sum(kernel * live_tile[:, None], axis=0), jnp.sum(kernel, axis=1))

    resident_part, visit_parts = lax.scan(
        tile_sums, jnp.zeros((residents.shape[0],), jnp.float32), (visit_blocks, live_blocks)
    )
    return (visit_parts.reshape(count_rows), resident_part)


def on_device(resident, ingest, cluster_ids):
    cycle_size = lax.axis_size("blk")
    slot_count = 3 * INGEST_DEV // (2 * cycle_size)
    columns = ingest.shape[1]
    owners = cluster_ids // CL_OWN
    onehot = (owners[:, None] == jnp.arange(cycle_size, dtype=jnp.int32)[None, :]).astype(jnp.int32)
    rank_within = jnp.sum((jnp.cumsum(onehot, axis=0) - onehot) * onehot, axis=1)
    targets = owners * slot_count + rank_within
    unit_ingest = unit_rows(ingest)
    outgoing = (
        jnp.zeros((cycle_size * slot_count, columns), jnp.bfloat16).at[targets].set(unit_ingest)
    )
    filled = (
        jnp.zeros((cycle_size * slot_count,), jnp.bfloat16)
        .at[targets]
        .set(jnp.ones((ingest.shape[0],), jnp.bfloat16))
    )
    arrived, present = (
        lax.all_to_all(
            outgoing.reshape(cycle_size, slot_count, columns),
            "blk",
            split_axis=0,
            concat_axis=0,
            tiled=True,
        ),
        lax.all_to_all(
            filled.reshape(cycle_size, slot_count), "blk", split_axis=0, concat_axis=0, tiled=True
        ),
    )
    visitors, marked = (
        lax.all_gather(
            arrived.reshape(cycle_size * slot_count, columns), "rep", axis=0, tiled=True
        ),
        lax.all_gather(present.reshape(cycle_size * slot_count), "rep", axis=0, tiled=True),
    )
    unit_resident = unit_rows(resident)
    visit_total = jnp.zeros((visitors.shape[0],), jnp.float32)
    resident_total = jnp.zeros((resident.shape[0],), jnp.float32)
    moving = unit_resident
    for rotation in range(CYCLE_STEPS + 1):
        if rotation > 0:
            moving = shifted(moving, "blk", -1)
            resident_total = shifted(resident_total, "blk", -1)
        visit_part, resident_part = kernel_sums(visitors, marked, moving)
        visit_total = visit_total + visit_part
        resident_total = resident_total + resident_part
    resident_total = shifted(resident_total, "blk", CYCLE_STEPS)
    own_sums = lax.psum_scatter(visit_total, "rep", scatter_dimension=0, tiled=True)
    returned = lax.all_to_all(
        own_sums.reshape(cycle_size, slot_count), "blk", split_axis=0, concat_axis=0, tiled=True
    )
    density = returned.reshape(cycle_size * slot_count)[targets]
    return (jnp.log1p(resident_total), jnp.log1p(density))


PAIR = 2
LANES = 128
SUBLANES = 8
INGEST_CHUNK = 256
RESIDENT_CHUNK = 256
TILE = 512
MESH = pl.DeviceIdType.MESH


def dense_kernel(
    cycle, ids_ref, ingest_ref, resident_ref, resident_out, ingest_out,
    rows, bank, ids, by_resident, by_ingest, resident_sums, ingest_sums, resident_terms, ingest_terms,
    up_send, down_send, rows_recv, ids_send, ids_recv, peer_send, peer_recv, core_send, core_recv,
    relay_send, relay_recv, part_send, part_recv, term_send, term_recv,
):
    line_size = cycle // PAIR
    me = lax.axis_index("blk")
    core = lax.axis_index("rep")
    line, side = me // PAIR, me % PAIR
    chunks = ingest_ref.shape[0] // INGEST_CHUNK
    held = resident_ref.shape[0]
    pieces = held // RESIDENT_CHUNK
    tiles = held // TILE
    steps = (line_size - 1) * chunks

    def device(at_line, at_side, at_core):
        return {"blk": at_line * PAIR + at_side, "rep": at_core}

    sibling = device(line, side, 1 - core)
    peer = device(line, 1 - side, core)
    across = device(line, 1 - side, 1 - core)

    def remote(source, target, send, recv, where):
        return pltpu.make_async_remote_copy(
            src_ref=source, dst_ref=target, send_sem=send, recv_sem=recv, device_id=where, device_id_type=MESH
        )

    def up_copy(c):
        return remote(rows.at[c], rows.at[c], up_send.at[c], rows_recv.at[c], device(line + 1, side, core))

    def down_copy(c):
        return remote(rows.at[c], rows.at[c], down_send.at[c], rows_recv.at[c], device(line - 1, side, core))

    def peer_copy(m):
        return remote(
            bank.at[pl.ds(m * RESIDENT_CHUNK, RESIDENT_CHUNK)],
            bank.at[pl.ds(2 * held + m * RESIDENT_CHUNK, RESIDENT_CHUNK)],
            peer_send.at[m], peer_recv.at[m], peer,
        )

    def relay_copy(m):
        return remote(
            bank.at[pl.ds(2 * held + m * RESIDENT_CHUNK, RESIDENT_CHUNK)],
            bank.at[pl.ds(3 * held + m * RESIDENT_CHUNK, RESIDENT_CHUNK)],
            relay_send.at[m], relay_recv.at[m], sibling,
        )

    core_copy = remote(bank.at[pl.ds(0, held)], bank.at[pl.ds(held, held)], core_send, core_recv, sibling)

    def ids_copy(other):
        mine = ids.at[pl.ds(line * chunks, chunks)]
        return remote(mine, mine, ids_send.at[other], ids_recv.at[line], device(other, side, core))

    def ids_arrival(other):
        theirs = ids.at[pl.ds(other * chunks, chunks)]
        return remote(theirs, theirs, ids_send.at[other], ids_recv.at[other], device(other, side, core))

    def term_copy(other):
        return remote(
            ingest_sums.at[pl.ds(other * chunks, chunks)], ingest_terms.at[pl.ds(line * chunks, chunks)],
            term_send.at[other], term_recv.at[line], device(other, side, core),
        )

    def term_arrival(other):
        return remote(
            ingest_sums.at[pl.ds(other * chunks, chunks)], ingest_terms.at[pl.ds(other * chunks, chunks)],
            term_send.at[other], term_recv.at[other], device(other, side, core),
        )

    def part_copy(slot):
        return remote(
            resident_sums.at[slot], resident_terms.at[slot], part_send.at[slot], part_recv.at[slot],
            (None, sibling, peer, across)[slot],
        )

    barrier = pltpu.get_barrier_semaphore()
    for where in (sibling, peer, across):
        pl.semaphore_signal(barrier, inc=1, device_id=where, device_id_type=MESH)
    for hop in range(1, line_size):
        pl.semaphore_signal(
            barrier, inc=1, device_id=device((line + hop) % line_size, side, core), device_id_type=MESH
        )

    def unit(block):
        values = block.astype(jnp.float32)
        squares = jnp.sum(values * values, axis=-1, keepdims=True) + epsilon
        return (values * lax.rsqrt(squares)).astype(jnp.bfloat16)

    for j in range(chunks):
        rows[line * chunks + j] = unit(ingest_ref[j * INGEST_CHUNK:(j + 1) * INGEST_CHUNK, :])
        ids[line * chunks + j] = ids_ref[j]
    pl.semaphore_wait(barrier, line_size + 2)
    for j in range(chunks):
        @pl.when(line + 1 < line_size)
        def _():
            up_copy(line * chunks + j).start()

        @pl.when(line > 0)
        def _():
            down_copy(line * chunks + j).start()
    for hop in range(1, line_size):
        ids_copy((line + hop) % line_size).start()

    @pl.loop(0, pieces)
    def _(m):
        part = pl.ds(m * RESIDENT_CHUNK, RESIDENT_CHUNK)
        bank[part, :] = unit(resident_ref[part, :])

    for m in range(pieces):
        peer_copy(m).start()
    core_copy.start()
    by_resident[...] = jnp.zeros_like(by_resident)
    by_ingest[...] = jnp.zeros_like(by_ingest)
    for hop in range(1, line_size):
        ids_arrival((line + hop) % line_size).wait_recv()

    scale = math.log2(math.e) / temper
    span = CL_OWN * cycle

    def work(c, first, last):
        @pl.loop(first, last)
        def _(tile):
            part = pl.ds(tile * TILE, TILE)
            position = line * PAIR + jnp.where(tile < 2 * tiles, side, 1 - side)
            gap = (position + 1) * CL_OWN - 1 - ids[c]
            gap = jnp.where(gap < 0, gap + span, gap)
            bias = jnp.where(gap < CL_OWN * (CYCLE_STEPS + 1), -scale, -1e30)
            scores = lax.dot_general(
                bank[part, :], rows[c], (((1,), (1,)), ((), ())), preferred_element_type=jnp.float32
            )
            kernel = jnp.exp2(scores * scale + bias)
            by_ingest[c] += jnp.sum(kernel.reshape(TILE // SUBLANES, SUBLANES, INGEST_CHUNK), axis=0)
            folded = kernel[:, :LANES]
            for n in range(1, INGEST_CHUNK // LANES):
                folded = folded + kernel[:, n * LANES:(n + 1) * LANES]
            by_resident[part, :] += folded

    @pl.loop(0, 2)
    def _(half):
        @pl.when(half == 1)
        def _():
            core_copy.wait_recv()

        @pl.loop(0, chunks)
        def _(j):
            work(line * chunks + j, half * tiles, (half + 1) * tiles)

    @pl.loop(0, steps)
    def _(step):
        hop, j = step // chunks + 1, step % chunks

        @pl.when(line - hop >= 0)
        def _():
            c = (line - hop) * chunks + j
            up_copy(c).wait_recv()

            @pl.when(line + 1 < line_size)
            def _():
                up_copy(c).start()

        @pl.when(line + hop < line_size)
        def _():
            c = (line + hop) * chunks + j
            down_copy(c).wait_recv()

            @pl.when(line > 0)
            def _():
                down_copy(c).start()

        @pl.when(step < pieces)
        def _():
            peer_copy(step).wait_recv()
            relay_copy(step).start()

        @pl.loop(0, 2)
        def _(way):
            other = line + (2 * way - 1) * hop

            @pl.when((other >= 0) & (other < line_size))
            def _():
                work(other * chunks + j, 0, jnp.where(step < pieces, 2 * tiles, 4 * tiles))

        @pl.when(step == pieces - 1)
        def _():
            for m in range(pieces):
                relay_copy(m).wait_recv()

            @pl.loop(0, line_size * chunks)
            def _(c):
                away = jnp.abs(c // chunks - line)
                arrived = (away - 1) * chunks + c % chunks

                @pl.when((away == 0) | (arrived < pieces))
                def _():
                    work(c, 2 * tiles, 4 * tiles)

    ingest_sums[...] = jnp.sum(by_ingest[...], axis=1, keepdims=True)

    def gather_slot(slot):
        block = by_resident[slot * held:(slot + 1) * held, :]
        resident_sums[slot] = jnp.sum(block.T, axis=0, keepdims=True)

    for slot in (3, 2, 1):
        gather_slot(slot)
    for hop in range(1, line_size):
        term_copy((line + hop) % line_size).start()
    gather_slot(0)
    for slot in (3, 2, 1):
        part_copy(slot).start()

    for c in range(line_size * chunks):
        @pl.when((c // chunks <= line) & (line + 1 < line_size))
        def _():
            up_copy(c).wait_send()

        @pl.when((c // chunks >= line) & (line > 0))
        def _():
            down_copy(c).wait_send()
    for m in range(pieces):
        peer_copy(m).wait_send()
        relay_copy(m).wait_send()
    core_copy.wait_send()

    resident_total = resident_sums[0]
    for slot in (1, 2, 3):
        part_copy(slot).wait()
        resident_total = resident_total + resident_terms[slot]
    resident_out[...] = resident_total
    ingest_total = ingest_sums[pl.ds(line * chunks, chunks)]
    for hop in range(1, line_size):
        other = (line + hop) % line_size
        term_arrival(other).wait_recv()
        ingest_total = ingest_total + ingest_terms[pl.ds(other * chunks, chunks)]
    ingest_out[...] = ingest_total
    for hop in range(1, line_size):
        other = (line + hop) % line_size
        ids_copy(other).wait_send()
        term_copy(other).wait_send()


def dense_on_device(cycle, resident, ingest, cluster_ids):
    held, columns = resident.shape
    count = ingest.shape[0]
    chunks = count // INGEST_CHUNK
    blocks = cycle // PAIR * chunks
    line_size = cycle // PAIR
    pieces = held // RESIDENT_CHUNK
    dma = pltpu.SemaphoreType.DMA
    vmem = pl.BlockSpec(memory_space=pltpu.VMEM)
    resident_total, ingest_total = pl.pallas_call(
        functools.partial(dense_kernel, cycle),
        out_shape=(
            jax.ShapeDtypeStruct((1, held), jnp.float32),
            jax.ShapeDtypeStruct((chunks, 1, INGEST_CHUNK), jnp.float32),
        ),
        in_specs=[vmem] * 3,
        out_specs=(vmem, vmem),
        scratch_shapes=[
            pltpu.VMEM((blocks, INGEST_CHUNK, columns), jnp.bfloat16),
            pltpu.VMEM((4 * held, columns), jnp.bfloat16),
            pltpu.VMEM((blocks, 1, INGEST_CHUNK), jnp.int32),
            pltpu.VMEM((4 * held, LANES), jnp.float32),
            pltpu.VMEM((blocks, SUBLANES, INGEST_CHUNK), jnp.float32),
            pltpu.VMEM((4, 1, held), jnp.float32),
            pltpu.VMEM((blocks, 1, INGEST_CHUNK), jnp.float32),
            pltpu.VMEM((4, 1, held), jnp.float32),
            pltpu.VMEM((blocks, 1, INGEST_CHUNK), jnp.float32),
            dma((blocks,)), dma((blocks,)), dma((blocks,)),
            dma((line_size,)), dma((line_size,)),
            dma((pieces,)), dma((pieces,)),
            dma, dma,
            dma((pieces,)), dma((pieces,)),
            dma((4,)), dma((4,)),
            dma((line_size,)), dma((line_size,)),
        ],
        compiler_params=pltpu.CompilerParams(collective_id=0, has_side_effects=True),
    )(cluster_ids.reshape(chunks, 1, INGEST_CHUNK), ingest, resident)
    return (jnp.log1p(resident_total.reshape(held)), jnp.log1p(ingest_total.reshape(count)))


def solution(mesh):
    in_specs = (
        P(("groups", "blk", "rep"), None),
        P(("groups", "blk", "rep"), None),
        P(("groups", "blk", "rep")),
    )
    out_specs = (P(("groups", "blk", "rep")), P(("groups", "blk", "rep")))
    cycle = mesh.shape["blk"]
    dense = 2 * (CYCLE_STEPS + 1) >= cycle and cycle % PAIR == 0 and mesh.shape["rep"] == 2
    body = functools.partial(dense_on_device, cycle) if dense else on_device
    return jax.shard_map(
        body, mesh=mesh, in_specs=in_specs, out_specs=out_specs, check_vma=False
    )
```

```python
import functools
import math

import jax
import jax.numpy as jnp
from jax import lax
from jax.experimental import pallas as pl
from jax.experimental.pallas import tpu as pltpu
from jax.sharding import PartitionSpec as P

INGEST_DEV = 512
CL_OWN = 16
CYCLE_STEPS = 4


temper = 0.2
epsilon = 1e-06


def shifted(value, axis, steps):
    count = lax.axis_size(axis)
    pairs = [(source, (source + steps) % count) for source in range(count)]
    return lax.ppermute(value, axis, pairs)


def unit_rows(rows):
    values = rows.astype(jnp.float32)
    squares = jnp.sum(values * values, axis=-1, keepdims=True) + epsilon
    factor = lax.rsqrt(squares)
    return (values * factor).astype(jnp.bfloat16)


def kernel_sums(visitors, occupancy, residents):
    count_rows = visitors.shape[0]
    block_rows = 512
    num_blocks = count_rows // block_rows
    visit_blocks = visitors.reshape(num_blocks, block_rows, visitors.shape[1])
    live_blocks = occupancy.astype(jnp.float32).reshape(num_blocks, block_rows)

    def tile_sums(running, pieces):
        visit_tile, live_tile = pieces
        scores = jnp.einsum("vd,rd->vr", visit_tile, residents, preferred_element_type=jnp.float32)
        kernel = jnp.exp((scores - 1.0) / temper)
        return (running + jnp.sum(kernel * live_tile[:, None], axis=0), jnp.sum(kernel, axis=1))

    resident_part, visit_parts = lax.scan(
        tile_sums, jnp.zeros((residents.shape[0],), jnp.float32), (visit_blocks, live_blocks)
    )
    return (visit_parts.reshape(count_rows), resident_part)


def on_device(resident, ingest, cluster_ids):
    cycle_size = lax.axis_size("blk")
    slot_count = 3 * INGEST_DEV // (2 * cycle_size)
    columns = ingest.shape[1]
    owners = cluster_ids // CL_OWN
    onehot = (owners[:, None] == jnp.arange(cycle_size, dtype=jnp.int32)[None, :]).astype(jnp.int32)
    rank_within = jnp.sum((jnp.cumsum(onehot, axis=0) - onehot) * onehot, axis=1)
    targets = owners * slot_count + rank_within
    unit_ingest = unit_rows(ingest)
    outgoing = (
        jnp.zeros((cycle_size * slot_count, columns), jnp.bfloat16).at[targets].set(unit_ingest)
    )
    filled = (
        jnp.zeros((cycle_size * slot_count,), jnp.bfloat16)
        .at[targets]
        .set(jnp.ones((ingest.shape[0],), jnp.bfloat16))
    )
    arrived, present = (
        lax.all_to_all(
            outgoing.reshape(cycle_size, slot_count, columns),
            "blk",
            split_axis=0,
            concat_axis=0,
            tiled=True,
        ),
        lax.all_to_all(
            filled.reshape(cycle_size, slot_count), "blk", split_axis=0, concat_axis=0, tiled=True
        ),
    )
    visitors, marked = (
        lax.all_gather(
            arrived.reshape(cycle_size * slot_count, columns), "rep", axis=0, tiled=True
        ),
        lax.all_gather(present.reshape(cycle_size * slot_count), "rep", axis=0, tiled=True),
    )
    unit_resident = unit_rows(resident)
    visit_total = jnp.zeros((visitors.shape[0],), jnp.float32)
    resident_total = jnp.zeros((resident.shape[0],), jnp.float32)
    moving = unit_resident
    for rotation in range(CYCLE_STEPS + 1):
        if rotation > 0:
            moving = shifted(moving, "blk", -1)
            resident_total = shifted(resident_total, "blk", -1)
        visit_part, resident_part = kernel_sums(visitors, marked, moving)
        visit_total = visit_total + visit_part
        resident_total = resident_total + resident_part
    resident_total = shifted(resident_total, "blk", CYCLE_STEPS)
    own_sums = lax.psum_scatter(visit_total, "rep", scatter_dimension=0, tiled=True)
    returned = lax.all_to_all(
        own_sums.reshape(cycle_size, slot_count), "blk", split_axis=0, concat_axis=0, tiled=True
    )
    density = returned.reshape(cycle_size * slot_count)[targets]
    return (jnp.log1p(resident_total), jnp.log1p(density))


PAIR = 2
LANES = 128
SUBLANES = 8
INGEST_CHUNK = 256
RESIDENT_CHUNK = 256
TILE = 1024
MESH = pl.DeviceIdType.MESH


def dense_kernel(
    cycle, ids_ref, ingest_ref, resident_ref, resident_out, ingest_out,
    raw_ingest, raw_resident, load_sem, rows, bank, ids, by_resident, by_ingest, resident_sums, ingest_sums, resident_terms, ingest_terms,
    up_send, down_send, rows_recv, ids_send, ids_recv, peer_send, peer_recv, core_send, core_recv,
    relay_send, relay_recv, part_send, part_recv, term_send, term_recv,
):
    line_size = cycle // PAIR
    me = lax.axis_index("blk")
    core = lax.axis_index("rep")
    line, side = me // PAIR, me % PAIR
    chunks = ingest_ref.shape[0] // INGEST_CHUNK
    held = resident_ref.shape[0]
    pieces = held // RESIDENT_CHUNK
    tiles = held // TILE
    steps = (line_size - 1) * chunks

    def device(at_line, at_side, at_core):
        return {"blk": at_line * PAIR + at_side, "rep": at_core}

    sibling = device(line, side, 1 - core)
    peer = device(line, 1 - side, core)
    across = device(line, 1 - side, 1 - core)

    def remote(source, target, send, recv, where):
        return pltpu.make_async_remote_copy(
            src_ref=source, dst_ref=target, send_sem=send, recv_sem=recv, device_id=where, device_id_type=MESH
        )

    def up_copy(c):
        return remote(rows.at[c], rows.at[c], up_send.at[c], rows_recv.at[c], device(line + 1, side, core))

    def down_copy(c):
        return remote(rows.at[c], rows.at[c], down_send.at[c], rows_recv.at[c], device(line - 1, side, core))

    def peer_copy(m):
        return remote(
            bank.at[pl.ds(m * RESIDENT_CHUNK, RESIDENT_CHUNK)],
            bank.at[pl.ds(2 * held + m * RESIDENT_CHUNK, RESIDENT_CHUNK)],
            peer_send.at[m], peer_recv.at[m], peer,
        )

    def relay_copy(m):
        return remote(
            bank.at[pl.ds(2 * held + m * RESIDENT_CHUNK, RESIDENT_CHUNK)],
            bank.at[pl.ds(3 * held + m * RESIDENT_CHUNK, RESIDENT_CHUNK)],
            relay_send.at[m], relay_recv.at[m], sibling,
        )

    core_copy = remote(bank.at[pl.ds(0, held)], bank.at[pl.ds(held, held)], core_send, core_recv, sibling)

    def ids_copy(other):
        mine = ids.at[pl.ds(line * chunks, chunks)]
        return remote(mine, mine, ids_send.at[other], ids_recv.at[line], device(other, side, core))

    def ids_arrival(other):
        theirs = ids.at[pl.ds(other * chunks, chunks)]
        return remote(theirs, theirs, ids_send.at[other], ids_recv.at[other], device(other, side, core))

    def term_copy(other):
        return remote(
            ingest_sums.at[pl.ds(other * chunks, chunks)], ingest_terms.at[pl.ds(line * chunks, chunks)],
            term_send.at[other], term_recv.at[line], device(other, side, core),
        )

    def term_arrival(other):
        return remote(
            ingest_sums.at[pl.ds(other * chunks, chunks)], ingest_terms.at[pl.ds(other * chunks, chunks)],
            term_send.at[other], term_recv.at[other], device(other, side, core),
        )

    def part_copy(slot):
        return remote(
            resident_sums.at[slot], resident_terms.at[slot], part_send.at[slot], part_recv.at[slot],
            (None, sibling, peer, across)[slot],
        )

    barrier = pltpu.get_barrier_semaphore()
    for where in (sibling, peer, across):
        pl.semaphore_signal(barrier, inc=1, device_id=where, device_id_type=MESH)
    for hop in range(1, line_size):
        pl.semaphore_signal(
            barrier, inc=1, device_id=device((line + hop) % line_size, side, core), device_id_type=MESH
        )

    ingest_load = pltpu.make_async_copy(ingest_ref, raw_ingest, load_sem.at[0])
    resident_load = pltpu.make_async_copy(resident_ref, raw_resident, load_sem.at[1])
    ids_load = pltpu.make_async_copy(ids_ref, ids.at[pl.ds(line * chunks, chunks)], load_sem.at[2])
    for load in (ingest_load, ids_load, resident_load):
        load.start()

    def unit(block):
        values = block.astype(jnp.float32)
        squares = jnp.sum(values * values, axis=-1, keepdims=True) + epsilon
        return (values * lax.rsqrt(squares)).astype(jnp.bfloat16)

    ingest_load.wait()
    for j in range(chunks):
        rows[line * chunks + j] = unit(raw_ingest[j * INGEST_CHUNK:(j + 1) * INGEST_CHUNK, :])
    ids_load.wait()
    pl.semaphore_wait(barrier, line_size + 2)
    for hop in range(1, line_size):
        ids_copy((line + hop) % line_size).start()
    for j in range(chunks):
        @pl.when(line + 1 < line_size)
        def _():
            up_copy(line * chunks + j).start()

        @pl.when(line > 0)
        def _():
            down_copy(line * chunks + j).start()

    resident_load.wait()

    @pl.loop(0, pieces)
    def _(m):
        part = pl.ds(m * RESIDENT_CHUNK, RESIDENT_CHUNK)
        bank[part, :] = unit(raw_resident[part, :])

    for m in range(pieces):
        peer_copy(m).start()
    core_copy.start()
    by_resident[...] = jnp.zeros_like(by_resident)
    by_ingest[...] = jnp.zeros_like(by_ingest)

    scale = math.log2(math.e) / temper
    span = CL_OWN * cycle

    def work(c, first, last):
        @pl.loop(first, last)
        def _(tile):
            part = pl.ds(tile * TILE, TILE)
            position = line * PAIR + jnp.where(tile < 2 * tiles, side, 1 - side)
            gap = (position + 1) * CL_OWN - 1 - ids[c]
            gap = jnp.where(gap < 0, gap + span, gap)
            bias = jnp.where(gap < CL_OWN * (CYCLE_STEPS + 1), -scale, -1e30)
            scores = lax.dot_general(
                bank[part, :], rows[c], (((1,), (1,)), ((), ())), preferred_element_type=jnp.float32
            )
            kernel = jnp.exp2(scores * scale + bias)
            by_ingest[c] += jnp.sum(kernel.reshape(TILE // SUBLANES, SUBLANES, INGEST_CHUNK), axis=0)
            folded = kernel[:, :LANES]
            for n in range(1, INGEST_CHUNK // LANES):
                folded = folded + kernel[:, n * LANES:(n + 1) * LANES]
            by_resident[part, :] += folded

    @pl.loop(0, 2)
    def _(half):
        @pl.when(half == 1)
        def _():
            core_copy.wait_recv()

        @pl.loop(0, chunks)
        def _(j):
            work(line * chunks + j, half * tiles, (half + 1) * tiles)

    for hop in range(1, line_size):
        ids_arrival((line + hop) % line_size).wait_recv()

    @pl.loop(0, steps)
    def _(step):
        hop, j = step // chunks + 1, step % chunks

        @pl.when(line - hop >= 0)
        def _():
            c = (line - hop) * chunks + j
            up_copy(c).wait_recv()

            @pl.when(line + 1 < line_size)
            def _():
                up_copy(c).start()

        @pl.when(line + hop < line_size)
        def _():
            c = (line + hop) * chunks + j
            down_copy(c).wait_recv()

            @pl.when(line > 0)
            def _():
                down_copy(c).start()

        @pl.when(step < pieces)
        def _():
            peer_copy(step).wait_recv()
            relay_copy(step).start()

        @pl.loop(0, 2)
        def _(way):
            other = line + (2 * way - 1) * hop

            @pl.when((other >= 0) & (other < line_size))
            def _():
                work(other * chunks + j, 0, jnp.where(step < pieces, 2 * tiles, 4 * tiles))

        @pl.when(step == pieces - 1)
        def _():
            for m in range(pieces):
                relay_copy(m).wait_recv()

            @pl.loop(0, line_size * chunks)
            def _(c):
                away = jnp.abs(c // chunks - line)
                arrived = (away - 1) * chunks + c % chunks

                @pl.when((away == 0) | (arrived < pieces))
                def _():
                    work(c, 2 * tiles, 4 * tiles)

    ingest_sums[...] = jnp.sum(by_ingest[...], axis=1, keepdims=True)

    def gather_slot(slot):
        block = by_resident[slot * held:(slot + 1) * held, :]
        resident_sums[slot] = jnp.sum(block.T, axis=0, keepdims=True)

    for slot in (3, 2, 1):
        gather_slot(slot)
    for hop in range(1, line_size):
        term_copy((line + hop) % line_size).start()
    gather_slot(0)
    for slot in (3, 2, 1):
        part_copy(slot).start()

    for c in range(line_size * chunks):
        @pl.when((c // chunks <= line) & (line + 1 < line_size))
        def _():
            up_copy(c).wait_send()

        @pl.when((c // chunks >= line) & (line > 0))
        def _():
            down_copy(c).wait_send()
    for m in range(pieces):
        peer_copy(m).wait_send()
        relay_copy(m).wait_send()
    core_copy.wait_send()

    resident_total = resident_sums[0]
    for slot in (1, 2, 3):
        part_copy(slot).wait()
        resident_total = resident_total + resident_terms[slot]
    resident_out[...] = resident_total
    ingest_total = ingest_sums[pl.ds(line * chunks, chunks)]
    for hop in range(1, line_size):
        other = (line + hop) % line_size
        term_arrival(other).wait_recv()
        ingest_total = ingest_total + ingest_terms[pl.ds(other * chunks, chunks)]
    ingest_out[...] = ingest_total
    for hop in range(1, line_size):
        other = (line + hop) % line_size
        ids_copy(other).wait_send()
        term_copy(other).wait_send()


def score_kernel(resident_total, ingest_total, resident_score, ingest_score):
    resident_score[...] = jnp.log1p(resident_total[...])
    ingest_score[...] = jnp.log1p(ingest_total[...])


def dense_on_device(cycle, resident, ingest, cluster_ids):
    held, columns = resident.shape
    count = ingest.shape[0]
    chunks = count // INGEST_CHUNK
    blocks = cycle // PAIR * chunks
    line_size = cycle // PAIR
    pieces = held // RESIDENT_CHUNK
    dma = pltpu.SemaphoreType.DMA
    vmem = pl.BlockSpec(memory_space=pltpu.VMEM)
    resident_total, ingest_total = pl.pallas_call(
        functools.partial(dense_kernel, cycle),
        out_shape=(
            jax.ShapeDtypeStruct((1, held), jnp.float32),
            jax.ShapeDtypeStruct((chunks, 1, INGEST_CHUNK), jnp.float32),
        ),
        in_specs=[pl.BlockSpec(memory_space=pl.ANY)] * 3,
        out_specs=(vmem, vmem),
        scratch_shapes=[
            pltpu.VMEM((count, columns), jnp.bfloat16),
            pltpu.VMEM((held, columns), jnp.bfloat16),
            dma((3,)),
            pltpu.VMEM((blocks, INGEST_CHUNK, columns), jnp.bfloat16),
            pltpu.VMEM((4 * held, columns), jnp.bfloat16),
            pltpu.VMEM((blocks, 1, INGEST_CHUNK), jnp.int32),
            pltpu.VMEM((4 * held, LANES), jnp.float32),
            pltpu.VMEM((blocks, SUBLANES, INGEST_CHUNK), jnp.float32),
            pltpu.VMEM((4, 1, held), jnp.float32),
            pltpu.VMEM((blocks, 1, INGEST_CHUNK), jnp.float32),
            pltpu.VMEM((4, 1, held), jnp.float32),
            pltpu.VMEM((blocks, 1, INGEST_CHUNK), jnp.float32),
            dma((blocks,)), dma((blocks,)), dma((blocks,)),
            dma((line_size,)), dma((line_size,)),
            dma((pieces,)), dma((pieces,)),
            dma, dma,
            dma((pieces,)), dma((pieces,)),
            dma((4,)), dma((4,)),
            dma((line_size,)), dma((line_size,)),
        ],
        compiler_params=pltpu.CompilerParams(collective_id=0, has_side_effects=True),
    )(cluster_ids.reshape(chunks, 1, INGEST_CHUNK), ingest, resident)
    resident_score, ingest_score = pl.pallas_call(
        score_kernel,
        out_shape=(
            jax.ShapeDtypeStruct(resident_total.shape, jnp.float32),
            jax.ShapeDtypeStruct(ingest_total.shape, jnp.float32),
        ),
        in_specs=[vmem] * 2,
        out_specs=(vmem, vmem),
    )(resident_total, ingest_total)
    return (resident_score.reshape(held), ingest_score.reshape(count))


def solution(mesh):
    in_specs = (
        P(("groups", "blk", "rep"), None),
        P(("groups", "blk", "rep"), None),
        P(("groups", "blk", "rep")),
    )
    out_specs = (P(("groups", "blk", "rep")), P(("groups", "blk", "rep")))
    cycle = mesh.shape["blk"]
    dense = 2 * (CYCLE_STEPS + 1) >= cycle and cycle % PAIR == 0 and mesh.shape["rep"] == 2
    body = functools.partial(dense_on_device, cycle) if dense else on_device
    return jax.shard_map(
        body, mesh=mesh, in_specs=in_specs, out_specs=out_specs, check_vma=False
    )
```

```python
import functools
import math

import jax
import jax.numpy as jnp
from jax import lax
from jax.experimental import pallas as pl
from jax.experimental.pallas import tpu as pltpu
from jax.sharding import PartitionSpec as P

INGEST_DEV = 512
CL_OWN = 16
CYCLE_STEPS = 4


temper = 0.2
epsilon = 1e-06


def shifted(value, axis, steps):
    count = lax.axis_size(axis)
    pairs = [(source, (source + steps) % count) for source in range(count)]
    return lax.ppermute(value, axis, pairs)


def unit_rows(rows):
    values = rows.astype(jnp.float32)
    squares = jnp.sum(values * values, axis=-1, keepdims=True) + epsilon
    factor = lax.rsqrt(squares)
    return (values * factor).astype(jnp.bfloat16)


def kernel_sums(visitors, occupancy, residents):
    count_rows = visitors.shape[0]
    block_rows = 512
    num_blocks = count_rows // block_rows
    visit_blocks = visitors.reshape(num_blocks, block_rows, visitors.shape[1])
    live_blocks = occupancy.astype(jnp.float32).reshape(num_blocks, block_rows)

    def tile_sums(running, pieces):
        visit_tile, live_tile = pieces
        scores = jnp.einsum("vd,rd->vr", visit_tile, residents, preferred_element_type=jnp.float32)
        kernel = jnp.exp((scores - 1.0) / temper)
        return (running + jnp.sum(kernel * live_tile[:, None], axis=0), jnp.sum(kernel, axis=1))

    resident_part, visit_parts = lax.scan(
        tile_sums, jnp.zeros((residents.shape[0],), jnp.float32), (visit_blocks, live_blocks)
    )
    return (visit_parts.reshape(count_rows), resident_part)


def on_device(resident, ingest, cluster_ids):
    cycle_size = lax.axis_size("blk")
    slot_count = 3 * INGEST_DEV // (2 * cycle_size)
    columns = ingest.shape[1]
    owners = cluster_ids // CL_OWN
    onehot = (owners[:, None] == jnp.arange(cycle_size, dtype=jnp.int32)[None, :]).astype(jnp.int32)
    rank_within = jnp.sum((jnp.cumsum(onehot, axis=0) - onehot) * onehot, axis=1)
    targets = owners * slot_count + rank_within
    unit_ingest = unit_rows(ingest)
    outgoing = (
        jnp.zeros((cycle_size * slot_count, columns), jnp.bfloat16).at[targets].set(unit_ingest)
    )
    filled = (
        jnp.zeros((cycle_size * slot_count,), jnp.bfloat16)
        .at[targets]
        .set(jnp.ones((ingest.shape[0],), jnp.bfloat16))
    )
    arrived, present = (
        lax.all_to_all(
            outgoing.reshape(cycle_size, slot_count, columns),
            "blk",
            split_axis=0,
            concat_axis=0,
            tiled=True,
        ),
        lax.all_to_all(
            filled.reshape(cycle_size, slot_count), "blk", split_axis=0, concat_axis=0, tiled=True
        ),
    )
    visitors, marked = (
        lax.all_gather(
            arrived.reshape(cycle_size * slot_count, columns), "rep", axis=0, tiled=True
        ),
        lax.all_gather(present.reshape(cycle_size * slot_count), "rep", axis=0, tiled=True),
    )
    unit_resident = unit_rows(resident)
    visit_total = jnp.zeros((visitors.shape[0],), jnp.float32)
    resident_total = jnp.zeros((resident.shape[0],), jnp.float32)
    moving = unit_resident
    for rotation in range(CYCLE_STEPS + 1):
        if rotation > 0:
            moving = shifted(moving, "blk", -1)
            resident_total = shifted(resident_total, "blk", -1)
        visit_part, resident_part = kernel_sums(visitors, marked, moving)
        visit_total = visit_total + visit_part
        resident_total = resident_total + resident_part
    resident_total = shifted(resident_total, "blk", CYCLE_STEPS)
    own_sums = lax.psum_scatter(visit_total, "rep", scatter_dimension=0, tiled=True)
    returned = lax.all_to_all(
        own_sums.reshape(cycle_size, slot_count), "blk", split_axis=0, concat_axis=0, tiled=True
    )
    density = returned.reshape(cycle_size * slot_count)[targets]
    return (jnp.log1p(resident_total), jnp.log1p(density))


PAIR = 2
LANES = 128
SUBLANES = 8
INGEST_CHUNK = 256
RESIDENT_CHUNK = 256
TILE = 1024
MESH = pl.DeviceIdType.MESH


def dense_kernel(
    cycle, ids_ref, ingest_ref, resident_ref, resident_out, ingest_out,
    raw_ingest, raw_resident, load_sem, rows, bank, ids, by_resident, by_ingest, resident_sums, ingest_sums, resident_terms, ingest_terms,
    up_send, down_send, rows_recv, ids_send, ids_recv, peer_send, peer_recv, core_send, core_recv,
    relay_send, relay_recv, part_send, part_recv, term_send, term_recv,
):
    line_size = cycle // PAIR
    me = lax.axis_index("blk")
    core = lax.axis_index("rep")
    line, side = me // PAIR, me % PAIR
    chunks = ingest_ref.shape[0] // INGEST_CHUNK
    held = resident_ref.shape[0]
    pieces = held // RESIDENT_CHUNK
    tiles = held // TILE
    steps = (line_size - 1) * chunks

    def device(at_line, at_side, at_core):
        return {"blk": at_line * PAIR + at_side, "rep": at_core}

    sibling = device(line, side, 1 - core)
    peer = device(line, 1 - side, core)
    across = device(line, 1 - side, 1 - core)

    def remote(source, target, send, recv, where):
        return pltpu.make_async_remote_copy(
            src_ref=source, dst_ref=target, send_sem=send, recv_sem=recv, device_id=where, device_id_type=MESH
        )

    def up_copy(c):
        return remote(rows.at[c], rows.at[c], up_send.at[c], rows_recv.at[c], device(line + 1, side, core))

    def down_copy(c):
        return remote(rows.at[c], rows.at[c], down_send.at[c], rows_recv.at[c], device(line - 1, side, core))

    def peer_copy(m):
        return remote(
            bank.at[pl.ds(m * RESIDENT_CHUNK, RESIDENT_CHUNK)],
            bank.at[pl.ds(2 * held + m * RESIDENT_CHUNK, RESIDENT_CHUNK)],
            peer_send.at[m], peer_recv.at[m], peer,
        )

    def relay_copy(m):
        return remote(
            bank.at[pl.ds(2 * held + m * RESIDENT_CHUNK, RESIDENT_CHUNK)],
            bank.at[pl.ds(3 * held + m * RESIDENT_CHUNK, RESIDENT_CHUNK)],
            relay_send.at[m], relay_recv.at[m], sibling,
        )

    core_copy = remote(bank.at[pl.ds(0, held)], bank.at[pl.ds(held, held)], core_send, core_recv, sibling)

    def ids_copy(other):
        mine = ids.at[pl.ds(line * chunks, chunks)]
        return remote(mine, mine, ids_send.at[other], ids_recv.at[line], device(other, side, core))

    def ids_arrival(other):
        theirs = ids.at[pl.ds(other * chunks, chunks)]
        return remote(theirs, theirs, ids_send.at[other], ids_recv.at[other], device(other, side, core))

    def term_copy(other):
        return remote(
            ingest_sums.at[pl.ds(other * chunks, chunks)], ingest_terms.at[pl.ds(line * chunks, chunks)],
            term_send.at[other], term_recv.at[line], device(other, side, core),
        )

    def term_arrival(other):
        return remote(
            ingest_sums.at[pl.ds(other * chunks, chunks)], ingest_terms.at[pl.ds(other * chunks, chunks)],
            term_send.at[other], term_recv.at[other], device(other, side, core),
        )

    def part_copy(slot):
        return remote(
            resident_sums.at[slot], resident_terms.at[slot], part_send.at[slot], part_recv.at[slot],
            (None, sibling, peer, across)[slot],
        )

    barrier = pltpu.get_barrier_semaphore()
    for where in (sibling, peer, across):
        pl.semaphore_signal(barrier, inc=1, device_id=where, device_id_type=MESH)
    for hop in range(1, line_size):
        pl.semaphore_signal(
            barrier, inc=1, device_id=device((line + hop) % line_size, side, core), device_id_type=MESH
        )

    ingest_load = pltpu.make_async_copy(ingest_ref, raw_ingest, load_sem.at[0])
    resident_load = pltpu.make_async_copy(resident_ref, raw_resident, load_sem.at[1])
    ids_load = pltpu.make_async_copy(ids_ref, ids.at[pl.ds(line * chunks, chunks)], load_sem.at[2])
    for load in (ingest_load, ids_load, resident_load):
        load.start()

    def unit(block):
        values = block.astype(jnp.float32)
        squares = jnp.sum(values * values, axis=-1, keepdims=True) + epsilon
        return (values * lax.rsqrt(squares)).astype(jnp.bfloat16)

    ingest_load.wait()
    for j in range(chunks):
        rows[line * chunks + j] = unit(raw_ingest[j * INGEST_CHUNK:(j + 1) * INGEST_CHUNK, :])
    ids_load.wait()
    pl.semaphore_wait(barrier, line_size + 2)
    for hop in range(1, line_size):
        ids_copy((line + hop) % line_size).start()
    for j in range(chunks):
        @pl.when(line + 1 < line_size)
        def _():
            up_copy(line * chunks + j).start()

        @pl.when(line > 0)
        def _():
            down_copy(line * chunks + j).start()

    resident_load.wait()

    @pl.loop(0, pieces)
    def _(m):
        part = pl.ds(m * RESIDENT_CHUNK, RESIDENT_CHUNK)
        bank[part, :] = unit(raw_resident[part, :])

    for m in range(pieces):
        peer_copy(m).start()
    core_copy.start()
    by_resident[...] = jnp.zeros_like(by_resident)
    by_ingest[...] = jnp.zeros_like(by_ingest)

    scale = math.log2(math.e) / temper
    span = CL_OWN * cycle

    def work(c, first, last):
        @pl.loop(first, last)
        def _(tile):
            part = pl.ds(tile * TILE, TILE)
            position = line * PAIR + jnp.where(tile < 2 * tiles, side, 1 - side)
            gap = (position + 1) * CL_OWN - 1 - ids[c]
            gap = jnp.where(gap < 0, gap + span, gap)
            bias = jnp.where(gap < CL_OWN * (CYCLE_STEPS + 1), -scale, -1e30)
            scores = lax.dot_general(
                bank[part, :], rows[c], (((1,), (1,)), ((), ())), preferred_element_type=jnp.float32
            )
            kernel = jnp.exp2(scores * scale + bias)
            by_ingest[c] += jnp.sum(kernel.reshape(TILE // SUBLANES, SUBLANES, INGEST_CHUNK), axis=0)
            folded = kernel[:, :LANES]
            for n in range(1, INGEST_CHUNK // LANES):
                folded = folded + kernel[:, n * LANES:(n + 1) * LANES]
            by_resident[part, :] += folded

    @pl.loop(0, 2)
    def _(half):
        @pl.when(half == 1)
        def _():
            core_copy.wait_recv()

        @pl.loop(0, chunks)
        def _(j):
            work(line * chunks + j, half * tiles, (half + 1) * tiles)

    for hop in range(1, line_size):
        ids_arrival((line + hop) % line_size).wait_recv()

    @pl.loop(0, steps)
    def _(step):
        hop, j = step // chunks + 1, step % chunks

        @pl.when(line - hop >= 0)
        def _():
            c = (line - hop) * chunks + j
            up_copy(c).wait_recv()

            @pl.when(line + 1 < line_size)
            def _():
                up_copy(c).start()

        @pl.when(line + hop < line_size)
        def _():
            c = (line + hop) * chunks + j
            down_copy(c).wait_recv()

            @pl.when(line > 0)
            def _():
                down_copy(c).start()

        @pl.when(step < pieces)
        def _():
            peer_copy(step).wait_recv()
            relay_copy(step).start()

        @pl.loop(0, 2)
        def _(way):
            other = line + (2 * way - 1) * hop

            @pl.when((other >= 0) & (other < line_size))
            def _():
                work(other * chunks + j, 0, jnp.where(step < pieces, 2 * tiles, 4 * tiles))

        @pl.when(step == pieces - 1)
        def _():
            for m in range(pieces):
                relay_copy(m).wait_recv()

            @pl.loop(0, line_size * chunks)
            def _(c):
                away = jnp.abs(c // chunks - line)
                arrived = (away - 1) * chunks + c % chunks

                @pl.when((away == 0) | (arrived < pieces))
                def _():
                    work(c, 2 * tiles, 4 * tiles)

    ingest_sums[...] = jnp.sum(by_ingest[...], axis=1, keepdims=True)

    def gather_slot(slot):
        block = by_resident[slot * held:(slot + 1) * held, :]
        resident_sums[slot] = jnp.sum(block.T, axis=0, keepdims=True)

    gather_slot(3)
    for hop in range(1, line_size):
        term_copy((line + hop) % line_size).start()
    gather_slot(2)
    part_copy(3).start()
    gather_slot(1)
    part_copy(2).start()
    gather_slot(0)
    part_copy(1).start()

    for c in range(line_size * chunks):
        @pl.when((c // chunks <= line) & (line + 1 < line_size))
        def _():
            up_copy(c).wait_send()

        @pl.when((c // chunks >= line) & (line > 0))
        def _():
            down_copy(c).wait_send()
    for m in range(pieces):
        peer_copy(m).wait_send()
        relay_copy(m).wait_send()
    core_copy.wait_send()

    resident_total = resident_sums[0]
    for slot in (1, 2, 3):
        part_copy(slot).wait()
        resident_total = resident_total + resident_terms[slot]
    resident_out[...] = resident_total
    ingest_total = ingest_sums[pl.ds(line * chunks, chunks)]
    for hop in range(1, line_size):
        other = (line + hop) % line_size
        term_arrival(other).wait_recv()
        ingest_total = ingest_total + ingest_terms[pl.ds(other * chunks, chunks)]
    ingest_out[...] = ingest_total
    for hop in range(1, line_size):
        other = (line + hop) % line_size
        ids_copy(other).wait_send()
        term_copy(other).wait_send()


def score_kernel(resident_total, ingest_total, resident_score, ingest_score):
    resident_score[...] = jnp.log1p(resident_total[...])
    ingest_score[...] = jnp.log1p(ingest_total[...])


def dense_on_device(cycle, resident, ingest, cluster_ids):
    held, columns = resident.shape
    count = ingest.shape[0]
    chunks = count // INGEST_CHUNK
    blocks = cycle // PAIR * chunks
    line_size = cycle // PAIR
    pieces = held // RESIDENT_CHUNK
    dma = pltpu.SemaphoreType.DMA
    vmem = pl.BlockSpec(memory_space=pltpu.VMEM)
    resident_total, ingest_total = pl.pallas_call(
        functools.partial(dense_kernel, cycle),
        out_shape=(
            jax.ShapeDtypeStruct((1, held), jnp.float32),
            jax.ShapeDtypeStruct((chunks, 1, INGEST_CHUNK), jnp.float32),
        ),
        in_specs=[pl.BlockSpec(memory_space=pl.ANY)] * 3,
        out_specs=(vmem, vmem),
        scratch_shapes=[
            pltpu.VMEM((count, columns), jnp.bfloat16),
            pltpu.VMEM((held, columns), jnp.bfloat16),
            dma((3,)),
            pltpu.VMEM((blocks, INGEST_CHUNK, columns), jnp.bfloat16),
            pltpu.VMEM((4 * held, columns), jnp.bfloat16),
            pltpu.VMEM((blocks, 1, INGEST_CHUNK), jnp.int32),
            pltpu.VMEM((4 * held, LANES), jnp.float32),
            pltpu.VMEM((blocks, SUBLANES, INGEST_CHUNK), jnp.float32),
            pltpu.VMEM((4, 1, held), jnp.float32),
            pltpu.VMEM((blocks, 1, INGEST_CHUNK), jnp.float32),
            pltpu.VMEM((4, 1, held), jnp.float32),
            pltpu.VMEM((blocks, 1, INGEST_CHUNK), jnp.float32),
            dma((blocks,)), dma((blocks,)), dma((blocks,)),
            dma((line_size,)), dma((line_size,)),
            dma((pieces,)), dma((pieces,)),
            dma, dma,
            dma((pieces,)), dma((pieces,)),
            dma((4,)), dma((4,)),
            dma((line_size,)), dma((line_size,)),
        ],
        compiler_params=pltpu.CompilerParams(collective_id=0, has_side_effects=True),
    )(cluster_ids.reshape(chunks, 1, INGEST_CHUNK), ingest, resident)
    resident_score, ingest_score = pl.pallas_call(
        score_kernel,
        out_shape=(
            jax.ShapeDtypeStruct(resident_total.shape, jnp.float32),
            jax.ShapeDtypeStruct(ingest_total.shape, jnp.float32),
        ),
        in_specs=[vmem] * 2,
        out_specs=(vmem, vmem),
    )(resident_total, ingest_total)
    return (resident_score.reshape(held), ingest_score.reshape(count))


def solution(mesh):
    in_specs = (
        P(("groups", "blk", "rep"), None),
        P(("groups", "blk", "rep"), None),
        P(("groups", "blk", "rep")),
    )
    out_specs = (P(("groups", "blk", "rep")), P(("groups", "blk", "rep")))
    cycle = mesh.shape["blk"]
    dense = 2 * (CYCLE_STEPS + 1) >= cycle and cycle % PAIR == 0 and mesh.shape["rep"] == 2
    body = functools.partial(dense_on_device, cycle) if dense else on_device
    return jax.shard_map(
        body, mesh=mesh, in_specs=in_specs, out_specs=out_specs, check_vma=False
    )
```
